32 devices in a mesh: section: 16 (over z, y, x), tensor: 2 (over core).
Axes of the slice: x: 2, y: 2, z: 4, core: 2. Of those that a mesh axis runs over, the one named last changes fastest.
Arguments:
- hidden_in: bfloat16 [128, 8192], P(None, 'tensor'), may hold values from -36 to 36
- segment_ids: int32 [4, 32], replicated, may hold values from 0 to 7, never falling along the last dimension, each value on 1 to 8 neighbouring positions
- segment_job: int32 [4, 8], replicated, may hold values from 0 to 5
- job_adapter: int32 [6], replicated, may hold values from 0 to 3
- owner: int32 [16], P('section'), may hold values from 0 to 1
- frozen: bfloat16 [16, 8192, 4096], P('section', None, 'tensor'), may hold values from -0.0625 to 0.0625
- norm_gain: bfloat16 [16, 4096], P('section'), may hold values from 0.3984375 to 1.59375
- inbox_down: bfloat16 [16, 2, 4096, 128], P('section', 'tensor'), may hold values from -0.0625 to 0.0625
- inbox_up: bfloat16 [16, 2, 128, 4096], P('section', 'tensor'), may hold values from -1 to 1
Outputs:
- section_out: bfloat16 [16, 128, 4096], P('section', None, 'tensor')
The draws below stay inside these ranges and needn't reach their ends.
Inputs may be any that keep to these rules, and one draw needn't show every extreme that they name: `segment_ids`: within each micro-batch the segment numbers never fall, and each of the 8 segments has 1 to 8 tokens.
All inputs are finite; a program needn't handle non-finite values.
Results may differ from the reference program's by a relative error of at most 0.02.
Values may be sent and summed in bfloat16 or wider, within the bound.
A program may use at most 128 MiB of HBM per device.

```python
import math
import jax
import jax.numpy as jnp
import numpy as np
from jax import lax

D = 8192
R = 32
NEW = 4
JOBS = 6
MB = 4
MTOK = 32
SEGS = 8
TOK = 128
PIECE = 2048
SEG_MOST = 8
N_SECTION = 16
N_TENSOR = 2


def draw_hidden_in(key, part):
    base_key, col_key, row_key = jax.random.split(key, 3)
    col_scale = jnp.exp(jax.random.uniform(col_key, (1, D), jnp.float32, math.log(0.3), math.log(3.0)))
    row_scale = jnp.exp(jax.random.uniform(row_key, (TOK, 1), jnp.float32, math.log(0.3), math.log(3.0)))
    values = jnp.clip(jax.random.normal(base_key, (TOK, D), jnp.float32), -4.0, 4.0)
    return (values * col_scale * row_scale).astype(jnp.bfloat16)


def place_ends(result, stream_key, smallest, top_value):
    dims = result.shape
    index_at = [jax.random.randint(jax.random.fold_in(stream_key, axis), (), 0, dims[axis]) for axis in range(len(dims))]
    result = result.at[tuple(index_at)].set(smallest)
    longest = dims.index(max(dims))
    index_at[longest] = (index_at[longest] + 1) % dims[longest]
    return result.at[tuple(index_at)].set(top_value)


def steps_of(key, shape, shards, low, largest):
    def one(position, shards_of):
        draws = jax.random.uniform(jax.random.fold_in(jax.random.fold_in(key, 6), position), (shards_of,), jnp.float32, low / len(shards), largest / len(shards))
        return jnp.repeat(jnp.exp(draws), shape[position] // shards_of).reshape((-1,) + (1,) * (len(shape) - position - 1))

    loudness = one(*shards[0])
    for cut in shards[1:]:
        loudness = loudness * one(*cut)
    return loudness


def split_up(amount, total, reach, lean):
    weights = [(1 << 20) // math.isqrt(standing ** lean) + 1 for standing in range(2, amount + 1)]
    rest, holding = total - reach - (amount - 1), [1] * (amount - 1)
    while rest > 0:
        free = [i for i in range(amount - 1) if holding[i] < reach]
        whole, budget = sum([weights[i] for i in free]), rest
        for i in free:
            extra = min(reach - holding[i], max(1, budget * weights[i] // whole), rest)
            holding[i] = holding[i] + extra
            rest = rest - extra
    return np.array([reach] + holding)


def uneven_parts(stream_key, count, total, most, skew):
    if count == 2:
        one = jax.random.randint(stream_key, (), max(1, total - most), min(most, total - 1) + 1)
        return jnp.stack([one, total - one])
    lengths = jnp.asarray(split_up(count, total, most, skew), jnp.int32)
    couples = (count - 1) // 2
    giver, taker = lengths[1:1 + 2 * couples:2], lengths[2:2 + 2 * couples:2]
    room = jnp.minimum(giver - 1, most - taker)
    passed = jax.random.randint(jax.random.fold_in(stream_key, 1), (couples,), 0, 1 << 20) % (room + 1)
    lengths = lengths.at[1:1 + 2 * couples:2].set(giver - passed).at[2:2 + 2 * couples:2].set(taker + passed)
    return lengths[jax.random.permutation(jax.random.fold_in(stream_key, 2), count)]


def gaussian(stream_key, shape, scale, reach, cuts=(), kind=jnp.bfloat16):
    loudness = steps_of(stream_key, shape, cuts, -0.22, 0.18) if cuts else 1.0
    result = jax.random.normal(stream_key, shape, jnp.float32) * scale * loudness
    return jnp.minimum(jnp.maximum(result, -reach), reach).astype(kind)


def setup_inputs(seed: int = 0) -> dict:
    key_list = jax.random.split(jax.random.key(seed), 10)
    hidden_in = draw_hidden_in(jax.random.fold_in(key_list[9], 71), 0)
    segment_ids = jax.vmap(lambda own: jnp.searchsorted(jnp.cumsum(uneven_parts(own, SEGS, MTOK, SEG_MOST, 2)), jnp.arange(MTOK), side="right"))(jax.random.split(key_list[1], MB)).reshape((MB, MTOK)).astype(jnp.int32)
    segment_job = place_ends(jax.random.randint(key_list[2], (MB, SEGS), 0, JOBS), jax.random.fold_in(key_list[2], 1), 0, JOBS - 1).astype(jnp.int32)
    job_adapter = place_ends(jax.random.randint(key_list[3], (JOBS,), 0, NEW), jax.random.fold_in(key_list[3], 1), 0, NEW - 1).astype(jnp.int32)
    owner = place_ends(jax.random.randint(key_list[4], (N_SECTION,), 0, N_TENSOR), jax.random.fold_in(key_list[4], 1), 0, N_TENSOR - 1).astype(jnp.int32)
    frozen = gaussian(key_list[5], (N_SECTION, D, D // 2), D ** -0.5, 0.0625, ((0, 16), (2, 2)))
    norm_gain = jnp.clip(1.0 + 0.12 * jax.random.normal(key_list[6], (N_SECTION, D // 2), jnp.float32), 0.3984375, 1.59375).astype(jnp.bfloat16)
    inbox_down = gaussian(key_list[7], (N_SECTION, N_TENSOR, D // 2, NEW * R), D ** -0.5, 0.0625, ((0, 16), (1, 2)))
    inbox_up = gaussian(key_list[8], (N_SECTION, N_TENSOR, NEW * R, D // 2), R ** -0.5, 1.0, ((0, 16), (1, 2)))
    return dict(hidden_in=hidden_in, segment_ids=segment_ids, segment_job=segment_job, job_adapter=job_adapter, owner=owner, frozen=frozen, norm_gain=norm_gain, inbox_down=inbox_down, inbox_up=inbox_up)


epsilon = 1e-05

def alternate(lower_part, upper_part):
    lead_rows = lower_part.shape[0]
    blocks = jnp.stack([lower_part.reshape(lead_rows, N_TENSOR, PIECE), upper_part.reshape(lead_rows, N_TENSOR, PIECE)], axis=2)
    return blocks.reshape(lead_rows, 2 * N_TENSOR * PIECE)

def product(left, right):
    return jnp.dot(left, right, preferred_element_type=jnp.float32)

def reference(hidden_in, segment_ids, segment_job, job_adapter, owner, frozen, norm_gain, inbox_down, inbox_up):
    token_job = jnp.take_along_axis(segment_job, segment_ids, axis=1)
    token_adapter = jnp.take(job_adapter, token_job.reshape(TOK), axis=0)
    keep_mask = jnp.arange(NEW * R, dtype=jnp.int32)[None, :] // R == token_adapter[:, None]
    state_now = hidden_in
    pieces = []
    for section_level in range(N_SECTION // 2):
        low_index = 2 * section_level
        high_index = low_index + 1
        weight = alternate(frozen[low_index], frozen[high_index])
        down_rows = alternate(inbox_down[low_index, owner[low_index]].T, inbox_down[high_index, owner[high_index]].T).T
        up_cols = alternate(inbox_up[low_index, owner[low_index]], inbox_up[high_index, owner[high_index]])
        gain_row = alternate(norm_gain[low_index][None, :], norm_gain[high_index][None, :])[0]
        values = state_now.astype(jnp.float32)
        row_scale = lax.rsqrt(lax.optimization_barrier(jnp.mean(values * values, axis=1, keepdims=True)) + epsilon)
        normed = (values * row_scale * gain_row.astype(jnp.float32)).astype(jnp.bfloat16)
        projected = product(normed, down_rows)
        kept_rank = jnp.where(keep_mask, projected, 0.0).astype(jnp.bfloat16)
        state_now = (values + product(normed, weight) + product(kept_rank, up_cols)).astype(jnp.bfloat16)
        split_state = state_now.reshape(TOK, N_TENSOR, 2, PIECE)
        pieces.append(split_state[:, :, 0, :].reshape(TOK, N_TENSOR * PIECE))
        pieces.append(split_state[:, :, 1, :].reshape(TOK, N_TENSOR * PIECE))
    return jnp.stack(pieces, axis=0)
```

```python
import functools
import jax
import jax.numpy as jnp
from jax import lax
from jax.experimental import pallas as pl
from jax.experimental.pallas import tpu as pltpu
from jax.sharding import PartitionSpec as P

R = 32
MESH = pl.DeviceIdType.MESH
epsilon = 1e-05


def kernel(
    sections, tensors, units, rows, piece, chunks, ranks, jobs_of,
    hidden, ids, seg_job, job_ad, owner, frozen, gain, idown, iup,
    out,
    w, xbuf, xg, outbuf, gother, dbuf, ubuf, dsel, usel, lowbuf, kept, scale,
    wsem, xsem, psem, fsend, osend, hsem, dsem, usem, isend, gsem, lsem, lsend,
):
    levels = sections // 2
    step = piece // chunks
    full = 2 * tensors * piece
    segs, jobs = jobs_of
    s = lax.axis_index("section")
    t = lax.axis_index("tensor")
    h = lax.rem(s, 2)
    level = s // 2
    other = s + 1 - 2 * h
    b = 2 * t + h

    def peer(d):
        return lax.rem(t + d, tensors)

    def cols(c):
        return pl.ds(pl.multiple_of(c * step, step), step)

    def part(k):
        return pl.ds(pl.multiple_of(k * piece, piece), piece)

    def weight(c):
        return pltpu.make_async_copy(frozen.at[0, :, cols(c)], w.at[:, cols(c)], wsem.at[c])

    def remote(src, dst, send, recv, section, tensor):
        return pltpu.make_async_remote_copy(
            src_ref=src, dst_ref=dst, send_sem=send, recv_sem=recv,
            device_id=(section, tensor), device_id_type=MESH,
        )

    def landed(ref, sem):
        pltpu.make_async_copy(ref, ref, sem).wait()

    own_down = pltpu.make_async_copy(idown.at[0, 0, part(t), :], dbuf.at[t], dsem.at[t])
    own_up = pltpu.make_async_copy(iup.at[0, 0, :, part(t)], ubuf.at[t], usem.at[t])

    @pl.when(level == 0)
    def _():
        for hh in range(2):
            for c in range(chunks):
                def read(m, _, hh=hh, c=c):
                    slot = pl.ds(c * step, step)
                    pltpu.make_async_copy(
                        hidden.at[pl.ds(pl.multiple_of(m * rows, rows), rows), pl.ds(hh * piece + c * step, step)],
                        xbuf.at[m, 2 * t + hh, :, slot],
                        xsem.at[m, hh, c],
                    ).start()
                    return 0
                lax.fori_loop(0, units, read, 0)
    own_down.start()
    own_up.start()
    for c in range(chunks):
        weight(c).start()

    barrier = pltpu.get_barrier_semaphore()

    def greet(section, tensor):
        pl.semaphore_signal(barrier, inc=1, device_id=(section, tensor), device_id_type=MESH)

    for d in range(1, tensors):
        greet(s, peer(d))
    for d in range(tensors):
        greet(other, peer(d))

    @pl.when(level > 0)
    def _():
        greet(s - 2, t)
        greet(other - 2, t)

    @pl.when(level < levels - 1)
    def _():
        greet(s + 2, t)
        greet(other + 2, t)

    ends = (level > 0).astype(jnp.int32) + (level < levels - 1).astype(jnp.int32)
    pl.semaphore_wait(barrier, 2 * tensors - 1 + 2 * ends)

    def send_down(d):
        return remote(idown.at[0, 0, part(peer(d)), :], dbuf.at[t], isend.at[0, d], dsem.at[t], s, peer(d))

    def send_up(d):
        return remote(iup.at[0, 0, :, part(peer(d))], ubuf.at[t], isend.at[1, d], usem.at[t], s, peer(d))

    send_gain = remote(gain, gother, gsem.at[0], gsem.at[1], other, t)
    send_gain.start()
    for d in range(1, tensors):
        send_down(d).start()
        send_up(d).start()

    def forward(m, c, hh, d):
        ref = xbuf.at[m, 2 * t + hh, :, cols(c)]
        return remote(ref, ref, fsend.at[m, d, hh, c], psem.at[m, t, hh, c], s, peer(d))

    def forward_chunk(m, c):
        for hh in range(2):
            landed(xbuf.at[m, 2 * t + hh, :, cols(c)], xsem.at[m, hh, c])
            for d in range(1, tensors):
                forward(m, c, hh, d).start()

    def low_to(m, side, d):
        ref = lowbuf.at[m, b]
        section = s if side == 0 else other
        return remote(ref, ref, lsend.at[m, side, d], lsem.at[m, b], section, peer(d))

    def low_part(m):
        own = xbuf[m, b].astype(jnp.float32) * gain[0:1, part(t)].astype(jnp.float32)
        lowbuf[m, b] = jnp.dot(own.astype(jnp.bfloat16), dsel[...], preferred_element_type=jnp.float32)
        for side in range(2):
            for d in range(1 - side, tensors):
                low_to(m, side, d).start()

    def send_out(m, c, side):
        section = (s if side == 0 else other) + 2
        return remote(
            outbuf.at[m, :, cols(c)], xbuf.at[m, b, :, cols(c)],
            osend.at[m, side, c], xsem.at[m, h, c], section, t,
        )

    def write_out(m):
        return pltpu.make_async_copy(
            outbuf.at[m], out.at[0, pl.ds(pl.multiple_of(m * rows, rows), rows), :], hsem.at[m]
        )

    def first(c, _):
        forward_chunk(0, c)
        return 0

    own_down.wait()
    own_up.wait()
    for d in range(1, tensors):
        landed(dbuf.at[peer(d)], dsem.at[peer(d)])
        landed(ubuf.at[peer(d)], usem.at[peer(d)])
    who = owner[0]
    down, up = dbuf[0], ubuf[0]
    for k in range(1, tensors):
        down = jnp.where(who == k, dbuf[k], down)
        up = jnp.where(who == k, ubuf[k], up)
    dsel[...] = down
    usel[...] = up
    send_gain.wait_recv()
    lax.fori_loop(0, chunks, first, 0)
    low_part(0)

    def unit(m, _):
        for d in range(1, tensors):
            for hh in range(2):
                for c in range(chunks):
                    landed(xbuf.at[m, 2 * peer(d) + hh, :, pl.ds(c * step, step)], psem.at[m, peer(d), hh, c])
        total = jnp.zeros((rows, 1), jnp.float32)
        for k in range(2 * tensors):
            where_gain = pl.ds((k // 2) * piece, piece)
            near = gain[0:1, where_gain].astype(jnp.float32)
            far = gother[0:1, where_gain].astype(jnp.float32)
            x = xbuf[m, k].astype(jnp.float32)
            total += jnp.sum(x * x, axis=1, keepdims=True)
            xg[:, k * piece : (k + 1) * piece] = (x * jnp.where(h == k % 2, near, far)).astype(jnp.bfloat16)
        scale[...] = jnp.broadcast_to(lax.rsqrt(total / full + epsilon), scale.shape)

        def chunk(c, _):
            @pl.when(m == 0)
            def _():
                weight(c).wait()

            @pl.when(m + 1 < units)
            def _():
                forward_chunk(m + 1, c)

                @pl.when(c == chunks - 1)
                def _():
                    low_part(m + 1)

            main = jnp.dot(xg[...], w[:, cols(c)], preferred_element_type=jnp.float32)

            @pl.when(c == 0)
            def _():
                for side in range(2):
                    for d in range(1 - side, tensors):
                        blk = 2 * peer(d) + (h if side == 0 else 1 - h)
                        landed(lowbuf.at[m, blk], lsem.at[m, blk])
                low = lowbuf[m, 0]
                for k in range(1, 2 * tensors):
                    low = low + lowbuf[m, k]
                low = low * scale[:, 0:1]
                seg = ids[pl.ds(m, 1), :]
                slot = jnp.zeros_like(seg)
                for g in range(segs):
                    slot = jnp.where(seg == g, job_ad[seg_job[m, g]], slot)
                column = lax.broadcasted_iota(jnp.int32, (ranks, rows), 0) // R
                hit = jnp.where(column == slot, 1.0, 0.0).astype(jnp.bfloat16)
                eye = jnp.where(
                    lax.broadcasted_iota(jnp.int32, (rows, rows), 0)
                    == lax.broadcasted_iota(jnp.int32, (rows, rows), 1), 1.0, 0.0
                ).astype(jnp.bfloat16)
                mask = lax.dot_general(eye, hit, (((1,), (1,)), ((), ())), preferred_element_type=jnp.float32)
                kept[...] = jnp.where(mask > 0.5, low, 0.0).astype(jnp.bfloat16)

            adapted = jnp.dot(kept[...], usel[:, cols(c)], preferred_element_type=jnp.float32)
            fresh = xbuf[m, b, :, cols(c)].astype(jnp.float32) + main * scale[:, 0:1] + adapted
            outbuf[m, :, cols(c)] = fresh.astype(jnp.bfloat16)

            @pl.when(level < levels - 1)
            def _():
                for side in range(2):
                    send_out(m, c, side).start()
            return 0

        lax.fori_loop(0, chunks, chunk, 0)
        write_out(m).start()
        return 0

    lax.fori_loop(0, units, unit, 0)

    send_gain.wait_send()
    for d in range(1, tensors):
        send_down(d).wait_send()
        send_up(d).wait_send()

    def drain(m, _):
        for d in range(1, tensors):
            for hh in range(2):
                for c in range(chunks):
                    forward(m, c, hh, d).wait_send()
        for side in range(2):
            for d in range(1 - side, tensors):
                low_to(m, side, d).wait_send()

        @pl.when(level < levels - 1)
        def _():
            for side in range(2):
                for c in range(chunks):
                    send_out(m, c, side).wait_send()
        write_out(m).wait()
        return 0

    lax.fori_loop(0, units, drain, 0)


def local(
    hidden_in, segment_ids, segment_job, job_adapter, owner, frozen, norm_gain, inbox_down, inbox_up
):
    tensors = lax.axis_size("tensor")
    sections = lax.axis_size("section")
    units, rows = segment_ids.shape
    depth, piece = frozen.shape[1:]
    ranks = inbox_down.shape[3]
    chunks = max(1, min(4, piece // 256))
    step = piece // chunks
    bf16, f32 = jnp.bfloat16, jnp.float32
    anywhere = pl.BlockSpec(memory_space=pl.ANY)
    smem = pl.BlockSpec(memory_space=pltpu.SMEM)
    vmem = pl.BlockSpec(memory_space=pltpu.VMEM)
    dma = pltpu.SemaphoreType.DMA
    body = functools.partial(
        kernel, sections, tensors, units, rows, piece, chunks, ranks,
        (segment_job.shape[1], job_adapter.shape[0]),
    )
    return pl.pallas_call(
        body,
        out_shape=jax.ShapeDtypeStruct((1, units * rows, piece), bf16),
        in_specs=[anywhere, vmem, smem, smem, smem, anywhere, vmem, anywhere, anywhere],
        out_specs=anywhere,
        scratch_shapes=[
            pltpu.VMEM((depth, piece), bf16),
            pltpu.VMEM((units, 2 * tensors, rows, piece), bf16),
            pltpu.VMEM((rows, depth), bf16),
            pltpu.VMEM((units, rows, piece), bf16),
            pltpu.VMEM(norm_gain.shape, bf16),
            pltpu.VMEM((tensors, piece, ranks), bf16),
            pltpu.VMEM((tensors, ranks, piece), bf16),
            pltpu.VMEM((piece, ranks), bf16),
            pltpu.VMEM((ranks, piece), bf16),
            pltpu.VMEM((units, 2 * tensors, rows, ranks), f32),
            pltpu.VMEM((rows, ranks), bf16),
            pltpu.VMEM((rows, 128), f32),
            dma((chunks,)),
            dma((units, 2, chunks)),
            dma((units, tensors, 2, chunks)),
            dma((units, tensors, 2, chunks)),
            dma((units, 2, chunks)),
            dma((units,)),
            dma((tensors,)),
            dma((tensors,)),
            dma((2, tensors)),
            dma((2,)),
            dma((units, 2 * tensors)),
            dma((units, 2, tensors)),
        ],
        compiler_params=pltpu.CompilerParams(
            collective_id=0, has_side_effects=True, vmem_limit_bytes=60 * 2**20
        ),
    )(hidden_in, segment_ids, segment_job, job_adapter, owner, frozen, norm_gain, inbox_down, inbox_up)


def solution(mesh):
    return jax.shard_map(
        local,
        mesh=mesh,
        in_specs=(
            P(None, "tensor"),
            P(),
            P(),
            P(),
            P("section"),
            P("section", None, "tensor"),
            P("section", None),
            P("section", "tensor", None, None),
            P("section", "tensor", None, None),
        ),
        out_specs=P("section", None, "tensor"),
        check_vma=False,
    )
```

```python
import functools
import jax
import jax.numpy as jnp
from jax import lax
from jax.experimental import pallas as pl
from jax.experimental.pallas import tpu as pltpu
from jax.sharding import PartitionSpec as P

R = 32
MESH = pl.DeviceIdType.MESH
epsilon = 1e-05


def kernel(
    sections, tensors, units, rows, piece, chunks, ranks, jobs_of,
    hidden, ids, seg_job, job_ad, owner, frozen, gain, idown, iup,
    out,
    w, xbuf, xg, acc, outbuf, gother, dbuf, ubuf, dsel, usel, lowbuf, kept, square, scale,
    wsem, vsem, xsem, psem, fsend, osend, hsem, dsem, usem, isend, gsem, lsem, lsend,
):
    levels = sections // 2
    step = piece // chunks
    full = 2 * tensors * piece
    segs, jobs = jobs_of
    s = lax.axis_index("section")
    t = lax.axis_index("tensor")
    h = lax.rem(s, 2)
    level = s // 2
    other = s + 1 - 2 * h
    b = 2 * t + h

    def peer(d):
        return lax.rem(t + d, tensors)

    def cols(c):
        return pl.ds(pl.multiple_of(c * step, step), step)

    def part(k):
        return pl.ds(pl.multiple_of(k * piece, piece), piece)

    def near_rows(hh, c):
        return pl.ds(pl.multiple_of((2 * t + hh) * piece + c * step, step), step)

    def far_rows(d):
        return pl.ds(pl.multiple_of(2 * peer(d) * piece, piece), 2 * piece)

    def near_weight(hh, c):
        return pltpu.make_async_copy(frozen.at[0, near_rows(hh, c), :], w.at[near_rows(hh, c), :], wsem.at[hh, c])

    def far_weight(d, c):
        return pltpu.make_async_copy(
            frozen.at[0, far_rows(d), cols(c)], w.at[far_rows(d), cols(c)], vsem.at[d, c]
        )

    def remote(src, dst, send, recv, section, tensor):
        return pltpu.make_async_remote_copy(
            src_ref=src, dst_ref=dst, send_sem=send, recv_sem=recv,
            device_id=(section, tensor), device_id_type=MESH,
        )

    def landed(ref, sem):
        pltpu.make_async_copy(ref, ref, sem).wait()

    own_down = pltpu.make_async_copy(idown.at[0, 0, part(t), :], dbuf.at[t], dsem.at[t])
    own_up = pltpu.make_async_copy(iup.at[0, 0, :, part(t)], ubuf.at[t], usem.at[t])

    @pl.when(level == 0)
    def _():
        for hh in range(2):
            for c in range(chunks):
                def read(m, _, hh=hh, c=c):
                    slot = pl.ds(c * step, step)
                    pltpu.make_async_copy(
                        hidden.at[pl.ds(pl.multiple_of(m * rows, rows), rows), pl.ds(hh * piece + c * step, step)],
                        xbuf.at[m, 2 * t + hh, :, slot],
                        xsem.at[m, hh, c],
                    ).start()
                    return 0
                lax.fori_loop(0, units, read, 0)
    own_down.start()
    own_up.start()
    for c in range(chunks):
        for hh in range(2):
            near_weight(hh, c).start()
    for c in range(chunks):
        for d in range(1, tensors):
            far_weight(d, c).start()

    barrier = pltpu.get_barrier_semaphore()

    def greet(section, tensor):
        pl.semaphore_signal(barrier, inc=1, device_id=(section, tensor), device_id_type=MESH)

    for d in range(1, tensors):
        greet(s, peer(d))
    for d in range(tensors):
        greet(other, peer(d))

    @pl.when(level > 0)
    def _():
        greet(s - 2, t)
        greet(other - 2, t)

    @pl.when(level < levels - 1)
    def _():
        greet(s + 2, t)
        greet(other + 2, t)

    ends = (level > 0).astype(jnp.int32) + (level < levels - 1).astype(jnp.int32)
    pl.semaphore_wait(barrier, 2 * tensors - 1 + 2 * ends)

    def send_down(d):
        return remote(idown.at[0, 0, part(peer(d)), :], dbuf.at[t], isend.at[0, d], dsem.at[t], s, peer(d))

    def send_up(d):
        return remote(iup.at[0, 0, :, part(peer(d))], ubuf.at[t], isend.at[1, d], usem.at[t], s, peer(d))

    send_gain = remote(gain, gother, gsem.at[0], gsem.at[1], other, t)
    send_gain.start()
    for d in range(1, tensors):
        send_down(d).start()
        send_up(d).start()

    def forward(m, c, hh, d):
        ref = xbuf.at[m, 2 * t + hh, :, cols(c)]
        return remote(ref, ref, fsend.at[m, d, hh, c], psem.at[m, t, hh, c], s, peer(d))

    def forward_one(m, c, hh):
        landed(xbuf.at[m, 2 * t + hh, :, cols(c)], xsem.at[m, hh, c])
        for d in range(1, tensors):
            forward(m, c, hh, d).start()

    def low_to(m, side, d):
        ref = lowbuf.at[m, b]
        section = s if side == 0 else other
        return remote(ref, ref, lsend.at[m, side, d], lsem.at[m, b], section, peer(d))

    def low_part(m):
        own = xbuf[m, b].astype(jnp.float32) * gain[0:1, part(t)].astype(jnp.float32)
        lowbuf[m, b] = jnp.dot(own.astype(jnp.bfloat16), dsel[...], preferred_element_type=jnp.float32)
        for side in range(2):
            for d in range(1 - side, tensors):
                low_to(m, side, d).start()

    def send_out(m, c, side):
        section = (s if side == 0 else other) + 2
        return remote(
            outbuf.at[m, :, cols(c)], xbuf.at[m, b, :, cols(c)],
            osend.at[m, side, c], xsem.at[m, h, c], section, t,
        )

    def write_out(m):
        return pltpu.make_async_copy(
            outbuf.at[m], out.at[0, pl.ds(pl.multiple_of(m * rows, rows), rows), :], hsem.at[m]
        )

    def forward_chunk(m, c):
        forward_one(m, c, h)

        @pl.when(c == chunks - 1)
        def _():
            low_part(m)

        forward_one(m, c, 1 - h)

    def gained(x, k_side, where_gain):
        near = gain[0:1, where_gain].astype(jnp.float32)
        far = gother[0:1, where_gain].astype(jnp.float32)
        return (x * jnp.where(h == k_side, near, far)).astype(jnp.bfloat16)

    own_down.wait()
    own_up.wait()
    for d in range(1, tensors):
        landed(dbuf.at[peer(d)], dsem.at[peer(d)])
        landed(ubuf.at[peer(d)], usem.at[peer(d)])
    who = owner[0]
    down, up = dbuf[0], ubuf[0]
    for k in range(1, tensors):
        down = jnp.where(who == k, dbuf[k], down)
        up = jnp.where(who == k, ubuf[k], up)
    dsel[...] = down
    usel[...] = up
    send_gain.wait_recv()

    def unit(m, _):
        square[...] = jnp.zeros_like(square)
        acc[...] = jnp.zeros_like(acc)
        forward_chunk(m, 0)

        def near(c, _):
            @pl.when(c + 1 < chunks)
            def _():
                forward_chunk(m, c + 1)

            @pl.when(m == 0)
            def _():
                for hh in range(2):
                    near_weight(hh, c).wait()

            part_sum = acc[...]
            total = jnp.zeros((rows, 1), jnp.float32)
            for hh in range(2):
                x = xbuf[m, 2 * t + hh, :, cols(c)].astype(jnp.float32)
                total += jnp.sum(x * x, axis=1, keepdims=True)
                values = gained(x, hh, pl.ds(pl.multiple_of(t * piece + c * step, step), step))
                part_sum += jnp.dot(values, w[near_rows(hh, c), :], preferred_element_type=jnp.float32)
            acc[...] = part_sum
            square[...] += jnp.broadcast_to(total, square.shape)
            return 0

        lax.fori_loop(0, chunks, near, 0)

        total = square[:, 0:1]
        for d in range(1, tensors):
            for hh in range(2):
                for c in range(chunks):
                    landed(xbuf.at[m, 2 * peer(d) + hh, :, pl.ds(c * step, step)], psem.at[m, peer(d), hh, c])
                x = xbuf[m, 2 * peer(d) + hh].astype(jnp.float32)
                total += jnp.sum(x * x, axis=1, keepdims=True)
                xg[d - 1, :, hh * piece : (hh + 1) * piece] = gained(x, hh, part(peer(d)))
        scale[...] = jnp.broadcast_to(lax.rsqrt(total / full + epsilon), scale.shape)

        def chunk(c, _):
            @pl.when(m == 0)
            def _():
                for d in range(1, tensors):
                    far_weight(d, c).wait()

            main = acc[:, cols(c)]
            for d in range(1, tensors):
                main += jnp.dot(xg[d - 1], w[far_rows(d), cols(c)], preferred_element_type=jnp.float32)

            @pl.when(c == 0)
            def _():
                for side in range(2):
                    for d in range(1 - side, tensors):
                        blk = 2 * peer(d) + (h if side == 0 else 1 - h)
                        landed(lowbuf.at[m, blk], lsem.at[m, blk])
                low = lowbuf[m, 0]
                for k in range(1, 2 * tensors):
                    low = low + lowbuf[m, k]
                low = low * scale[:, 0:1]
                seg = ids[pl.ds(m, 1), :]
                slot = jnp.zeros_like(seg)
                for g in range(segs):
                    slot = jnp.where(seg == g, job_ad[seg_job[m, g]], slot)
                column = lax.broadcasted_iota(jnp.int32, (ranks, rows), 0) // R
                hit = jnp.where(column == slot, 1.0, 0.0).astype(jnp.bfloat16)
                eye = jnp.where(
                    lax.broadcasted_iota(jnp.int32, (rows, rows), 0)
                    == lax.broadcasted_iota(jnp.int32, (rows, rows), 1), 1.0, 0.0
                ).astype(jnp.bfloat16)
                mask = lax.dot_general(eye, hit, (((1,), (1,)), ((), ())), preferred_element_type=jnp.float32)
                kept[...] = jnp.where(mask > 0.5, low, 0.0).astype(jnp.bfloat16)

            adapted = jnp.dot(kept[...], usel[:, cols(c)], preferred_element_type=jnp.float32)
            fresh = xbuf[m, b, :, cols(c)].astype(jnp.float32) + main * scale[:, 0:1] + adapted
            outbuf[m, :, cols(c)] = fresh.astype(jnp.bfloat16)

            @pl.when(level < levels - 1)
            def _():
                for side in range(2):
                    send_out(m, c, side).start()
            return 0

        lax.fori_loop(0, chunks, chunk, 0)
        write_out(m).start()
        return 0

    lax.fori_loop(0, units, unit, 0)

    send_gain.wait_send()
    for d in range(1, tensors):
        send_down(d).wait_send()
        send_up(d).wait_send()

    def drain(m, _):
        for d in range(1, tensors):
            for hh in range(2):
                for c in range(chunks):
                    forward(m, c, hh, d).wait_send()
        for side in range(2):
            for d in range(1 - side, tensors):
                low_to(m, side, d).wait_send()

        @pl.when(level < levels - 1)
        def _():
            for side in range(2):
                for c in range(chunks):
                    send_out(m, c, side).wait_send()
        write_out(m).wait()
        return 0

    lax.fori_loop(0, units, drain, 0)


def local(
    hidden_in, segment_ids, segment_job, job_adapter, owner, frozen, norm_gain, inbox_down, inbox_up
):
    tensors = lax.axis_size("tensor")
    sections = lax.axis_size("section")
    units, rows = segment_ids.shape
    depth, piece = frozen.shape[1:]
    ranks = inbox_down.shape[3]
    chunks = max(1, min(2, piece // 256))
    step = piece // chunks
    bf16, f32 = jnp.bfloat16, jnp.float32
    anywhere = pl.BlockSpec(memory_space=pl.ANY)
    smem = pl.BlockSpec(memory_space=pltpu.SMEM)
    vmem = pl.BlockSpec(memory_space=pltpu.VMEM)
    dma = pltpu.SemaphoreType.DMA
    body = functools.partial(
        kernel, sections, tensors, units, rows, piece, chunks, ranks,
        (segment_job.shape[1], job_adapter.shape[0]),
    )
    return pl.pallas_call(
        body,
        out_shape=jax.ShapeDtypeStruct((1, units * rows, piece), bf16),
        in_specs=[anywhere, vmem, smem, smem, smem, anywhere, vmem, anywhere, anywhere],
        out_specs=anywhere,
        scratch_shapes=[
            pltpu.VMEM((depth, piece), bf16),
            pltpu.VMEM((units, 2 * tensors, rows, piece), bf16),
            pltpu.VMEM((max(1, tensors - 1), rows, 2 * piece), bf16),
            pltpu.VMEM((rows, piece), f32),
            pltpu.VMEM((units, rows, piece), bf16),
            pltpu.VMEM(norm_gain.shape, bf16),
            pltpu.VMEM((tensors, piece, ranks), bf16),
            pltpu.VMEM((tensors, ranks, piece), bf16),
            pltpu.VMEM((piece, ranks), bf16),
            pltpu.VMEM((ranks, piece), bf16),
            pltpu.VMEM((units, 2 * tensors, rows, ranks), f32),
            pltpu.VMEM((rows, ranks), bf16),
            pltpu.VMEM((rows, 128), f32),
            pltpu.VMEM((rows, 128), f32),
            dma((2, chunks)),
            dma((tensors, chunks)),
            dma((units, 2, chunks)),
            dma((units, tensors, 2, chunks)),
            dma((units, tensors, 2, chunks)),
            dma((units, 2, chunks)),
            dma((units,)),
            dma((tensors,)),
            dma((tensors,)),
            dma((2, tensors)),
            dma((2,)),
            dma((units, 2 * tensors)),
            dma((units, 2, tensors)),
        ],
        compiler_params=pltpu.CompilerParams(
            collective_id=0, has_side_effects=True, vmem_limit_bytes=60 * 2**20
        ),
    )(hidden_in, segment_ids, segment_job, job_adapter, owner, frozen, norm_gain, inbox_down, inbox_up)


def solution(mesh):
    return jax.shard_map(
        local,
        mesh=mesh,
        in_specs=(
            P(None, "tensor"),
            P(),
            P(),
            P(),
            P("section"),
            P("section", None, "tensor"),
            P("section", None),
            P("section", "tensor", None, None),
            P("section", "tensor", None, None),
        ),
        out_specs=P("section", None, "tensor"),
        check_vma=False,
    )
```
